32 devices in a mesh: rows: 8 (over z, y), par: 4 (over x, core).
Axes of the slice: x: 2, y: 2, z: 4, core: 2. Of those that a mesh axis runs over, the one named last changes fastest.
Arguments:
- base_a: bfloat16 [4, 64, 256], P(None, 'rows'), may hold values from -6 to 6
- base_b: bfloat16 [4, 64, 256], P(None, 'rows'), may hold values from -6 to 6
- input_scale: float32 [256], replicated, may hold values from 0.1 to 3
- layer_one: bfloat16 [256, 1024], replicated, may hold values from -0.375 to 0.375
- layer_two: bfloat16 [1024, 1024], replicated, may hold values from -0.1875 to 0.1875
- layer_three: bfloat16 [1024, 128], replicated, may hold values from -0.1875 to 0.1875
- swap_cols: int32 [256], P('par'), may hold values from 0 to 255, each once
- window_ends: int32 [4], replicated, may hold values from 32 to 64
Outputs:
- first_order: float32 [4, 256, 128], P(None, 'par')
- total_order: float32 [4, 256, 128], P(None, 'par')
- total_variance: float32 [4, 128], replicated
The draws below stay inside these ranges and needn't reach their ends.
Inputs may be any that keep to these rules, and one draw needn't show every extreme that they name: window w uses its rows 0 to window_ends[w] - 1. `swap_cols`: each column appears once.
All inputs are finite; a program needn't handle non-finite values.
Results may differ from the reference program's by a relative error of at most 0.0055.
The reference program's roundings to bfloat16 on the way (of `inputs_a`, `inputs_b`, `inputs_c`, `hidden_one` and `hidden_two`) count: a program that leaves them out, or rounds other values in their place, can miss the bound.
Values sent between devices are 32-bit elements; how exact they have to be, the bound alone decides.
A program may use at most 64 MiB of HBM per device.

```python
import math
import jax
import jax.numpy as jnp
from jax import lax

D = 256
HIDDEN_SIZE = 1024
OUTPUTS = 128
WINDOWS = 4
WINDOW_ROWS = 64


def place_ends(values, key, least, top_value):
    longest = values.shape.index(max(values.shape))
    spots = []
    for shift in (0, 1):
        where = [jax.random.randint(jax.random.fold_in(key, axis), (), 0, length) for axis, length in enumerate(values.shape)]
        where[longest] = (where[longest] + shift) % values.shape[longest]
        spots.append(tuple(where))
    return values.at[spots[0]].set(least).at[spots[1]].set(top_value)


def block_scale(stream_key, extent, split, low, largest):
    def one(axis_at, shards_of):
        steps = jax.random.uniform(jax.random.fold_in(jax.random.fold_in(stream_key, 6), axis_at), (shards_of,), jnp.float32, low / len(split), largest / len(split))
        return jnp.repeat(jnp.exp(steps), extent[axis_at] // shards_of).reshape((-1,) + (1,) * (len(extent) - axis_at - 1))

    level = one(*split[0])
    for cut in split[1:]:
        level = level * one(*cut)
    return level


def noise(key, extent, spread, reach, split=(), held_as=jnp.bfloat16):
    entries = jax.random.normal(key, extent, jnp.float32) * spread
    if len(split) > 0:
        entries = block_scale(key, extent, split, -0.22, 0.18) * entries
    return jnp.clip(entries, min=-reach, max=reach).astype(held_as)


def setup_inputs(seed: int = 0) -> dict:
    key_of = jax.random.split(jax.random.key(seed), 9)
    base_a = noise(key_of[0], (WINDOWS, WINDOW_ROWS, D), 1.0, 6.0, ((1, 8),))
    base_b = noise(key_of[1], (WINDOWS, WINDOW_ROWS, D), 1.0, 6.0, ((1, 8),))
    input_scale = jnp.clip(jnp.exp(jax.random.uniform(key_of[2], (D,), jnp.float32, math.log(0.1), math.log(3.0))), 0.1, 3.0)
    layer_one = noise(key_of[3], (D, HIDDEN_SIZE), D ** -0.5, 0.375)
    layer_two = noise(key_of[4], (HIDDEN_SIZE, HIDDEN_SIZE), HIDDEN_SIZE ** -0.5, 0.1875)
    layer_three = noise(key_of[5], (HIDDEN_SIZE, OUTPUTS), HIDDEN_SIZE ** -0.5, 0.1875)
    swap_cols = jax.random.permutation(key_of[6], D).astype(jnp.int32)
    window_ends = place_ends(jax.random.randint(key_of[7], (WINDOWS,), WINDOW_ROWS // 2, WINDOW_ROWS + 1), jax.random.fold_in(key_of[7], 1), WINDOW_ROWS // 2, WINDOW_ROWS).astype(jnp.int32)
    return {"base_a": base_a, "base_b": base_b, "input_scale": input_scale, "layer_one": layer_one, "layer_two": layer_two, "layer_three": layer_three, "swap_cols": swap_cols, "window_ends": window_ends}


def network_tail(first_pre, layer_two, layer_three):
    hidden_one = jax.nn.silu(first_pre).astype(jnp.bfloat16)
    second_pre = jnp.dot(hidden_one, layer_two, preferred_element_type=jnp.float32)
    hidden_two = jax.nn.silu(second_pre).astype(jnp.bfloat16)
    return jnp.dot(hidden_two, layer_three, preferred_element_type=jnp.float32)


def surrogate(inputs, layer_one, layer_two, layer_three):
    first_pre = jnp.dot(inputs, layer_one, preferred_element_type=jnp.float32)
    return network_tail(first_pre, layer_two, layer_three)


def merge_total(former, latter):
    counts = former[0] + latter[0]
    change = latter[1] - former[1]
    return (counts, former[1] + change * latter[0] / counts,
            former[2] + latter[2] + change * change * former[0] * latter[0] / counts)


def merge_groups(former, latter):
    counts = former[0] + latter[0]
    change_b = latter[1] - former[1]
    change_d = latter[2] - former[2]
    pair_weight = former[0] * latter[0] / counts
    return (counts, former[1] + change_b * latter[0] / counts, former[2] + change_d * latter[0] / counts,
            former[3] + latter[3] + change_d * change_d * pair_weight,
            former[4] + latter[4] + change_b * change_d * pair_weight)


def reference(base_a, base_b, input_scale, layer_one, layer_two, layer_three, swap_cols, window_ends):
    positions = jnp.arange(D, dtype=jnp.int32)
    row_ids = jnp.arange(WINDOW_ROWS, dtype=jnp.int32)
    firsts = []
    totals = []
    variances = []
    running_total = None
    running_groups = None
    for window in range(WINDOWS):
        inputs_a = (base_a[window].astype(jnp.float32) * input_scale).astype(jnp.bfloat16)
        inputs_b = (base_b[window].astype(jnp.float32) * input_scale).astype(jnp.bfloat16)
        usable = (row_ids < window_ends[window]).astype(jnp.float32)[:, None]
        counts = jnp.sum(usable)
        out_a = surrogate(inputs_a, layer_one, layer_two, layer_three)
        out_b = surrogate(inputs_b, layer_one, layer_two, layer_three)
        pooled_count = 2.0 * counts
        pooled_mean = jnp.sum(usable * (out_a + out_b), axis=0) / pooled_count
        dev_a = out_a - pooled_mean
        dev_b = out_b - pooled_mean
        pooled_spread = jnp.sum(usable * (dev_a * dev_a + dev_b * dev_b), axis=0)
        mean_b = jnp.sum(usable * out_b, axis=0) / counts
        centered_b = usable * (out_b - mean_b)

        def one_group(column):
            chosen = (positions == column)[None, :]
            inputs_c = jnp.where(chosen, inputs_b, inputs_a)
            differ = surrogate(inputs_c, layer_one, layer_two, layer_three) - out_a
            mean_d = jnp.sum(usable * differ, axis=0) / counts
            centered_d = usable * (differ - mean_d)
            return mean_d, jnp.sum(centered_d * centered_d, axis=0), jnp.sum(centered_b * centered_d, axis=0)

        mean_d, spread_d, cross = lax.map(one_group, swap_cols)
        total_state = (pooled_count, pooled_mean, pooled_spread)
        group_state = (counts, mean_b, mean_d, spread_d, cross)
        if window == 0:
            running_total = total_state
            running_groups = group_state
        else:
            running_total = merge_total(running_total, total_state)
            running_groups = merge_groups(running_groups, group_state)
        variance = running_total[2] / running_total[0]
        firsts.append(running_groups[4] / running_groups[0] / variance)
        totals.append(0.5 * (running_groups[3] / running_groups[0] + running_groups[2] * running_groups[2]) / variance)
        variances.append(variance)
    return jnp.stack(firsts), jnp.stack(totals), jnp.stack(variances)
```

```python
import functools

import jax
import jax.numpy as jnp
from jax import lax
from jax.experimental import pallas as pl
from jax.experimental.pallas import tpu as pltpu
from jax.sharding import PartitionSpec as P

F32 = jnp.float32
BF16 = jnp.bfloat16
MESH = pl.DeviceIdType.MESH


def silu_of_half(half):
    return half + half * jnp.tanh(half)


def dot(x, y):
    return jnp.dot(x, y, preferred_element_type=F32)


def dot_t(x, y):
    return lax.dot_general(x, y, (((1,), (1,)), ((), ())), preferred_element_type=F32)


def flip(index, bit):
    return index + bit - 2 * bit * lax.rem(index // bit, 2)


def partner(me, k, n):
    other = me
    bit = 1
    while bit < n:
        if k & bit:
            other = flip(other, bit)
        bit *= 2
    return other


def near_plan(n):
    order = list(range(n // 2 - 1, -1, -1))
    head = max(1, len(order) // 4)
    return [order[:head], order[head:]]


def stage_count(gq):
    return 2 if gq % 2 == 0 else 1


def kernel(n, share, a_hbm, b_hbm, scale_hbm, cols_hbm, ends_hbm, w1_hbm, w2_hbm, w3_hbm,
           res, variance_ref,
           base_a, base_b, scale, cols, ends, w1, w2, w3,
           a_send, a_far, d_send, d_far, onehot, swapped, bt_send, bt_far, t_near,
           st_send, st_near, acc, pre_s, oa_s, h1, h2,
           in_sems, a_ss, a_rs, af_ss, d_ss, d_rs, b_ss, b_rs, bf_ss, t_ss, t_rs, s_ss, s_rs, r_ss, r_rs):
    windows, window_rows, width = base_a.shape
    stages, gh = res.shape[1], res.shape[3] // 2
    gq = stages * gh
    padded = onehot.shape[1]
    hidden = w2.shape[0]
    outputs = w3.shape[1]
    rows = windows * window_rows
    half = n // 2
    quarter = n // 4
    me = lax.axis_index("rows")
    if share:
        par = lax.axis_index("par")
        core = lax.rem(par, 2)
        mate = {"par": flip(par, 1)}

    barrier = pltpu.get_barrier_semaphore()
    for k in range(1, n):
        pl.semaphore_signal(barrier, inc=1, device_id={"rows": partner(me, k, n)}, device_id_type=MESH)
    if share:
        pl.semaphore_signal(barrier, inc=1, device_id=mate, device_id_type=MESH)

    pairs = ((a_hbm, base_a), (b_hbm, base_b), (scale_hbm, scale), (cols_hbm, cols), (ends_hbm, ends),
             (w1_hbm, w1), (w2_hbm, w2), (w3_hbm, w3))
    loads = [pltpu.make_async_copy(src, dst, in_sems.at[i]) for i, (src, dst) in enumerate(pairs)]
    for load in loads:
        load.start()

    def remote(src, dst, ss, rs, peer):
        return pltpu.make_async_remote_copy(
            src_ref=src, dst_ref=dst, send_sem=ss, recv_sem=rs, device_id=peer, device_id_type=MESH)

    def far_block(mine, j):
        if not share:
            slot = j if mine else quarter + j
            return slot, partner(me, half + slot, n)
        side = core if mine else 1 - core
        other = partner(me, half + j, n)
        return quarter * side + j, other + side * (flip(other, quarter) - other)

    first = [far_block(True, j) for j in range(quarter)]
    second = [far_block(False, j) for j in range(quarter)]
    direct = first if share else first + second

    for load in loads[:5]:
        load.wait()
    factor = scale[...]
    own_a32 = (base_a[...].reshape(rows, width).astype(F32) * factor).astype(BF16).astype(F32)
    own_a = own_a32.astype(BF16)
    own_b = (base_b[...].reshape(rows, width).astype(F32) * factor).astype(BF16)
    a_send[...] = own_a32
    lane = lax.broadcasted_iota(jnp.int32, (padded, width), 1)
    sub = lax.broadcasted_iota(jnp.int32, (padded, width), 0)
    for r in range(n):
        wanted = jnp.full((padded, width), cols[r * gq], jnp.int32)
        for g in range(1, gq):
            wanted = jnp.where(sub == g, cols[r * gq + g], wanted)
        onehot[r] = (lane == wanted).astype(F32)
    marks = onehot[...].reshape(n * padded, width).astype(BF16)
    d_send[...] = (0.5 * (dot_t(marks, own_b) - dot_t(marks, own_a))).reshape(n, padded, rows)

    pl.semaphore_wait(barrier, n if share else n - 1)
    a_copies = [remote(a_send, a_far.at[slot], a_ss.at[i], a_rs.at[slot], {"rows": peer})
                for i, (slot, peer) in enumerate(direct)]
    for copy in a_copies:
        copy.start()
    d_copies = []
    for k in range(half, n):
        peer = partner(me, k, n)
        d_copies.append(remote(d_send.at[peer], d_far.at[k - half], d_ss.at[k - half], d_rs.at[k - half],
                               {"rows": peer}))
        d_copies[-1].start()

    loads[5].wait()
    mark_near = jnp.concatenate([onehot[partner(me, k, n)] for k in range(half)], 0).astype(BF16)
    swapped[...] = dot(mark_near, w1[...]).reshape(half, padded, hidden)
    pre_ab = 0.5 * dot(jnp.concatenate([own_a, own_b], 0), w1[...])
    pre_a = pre_ab[:rows]

    def tail(count):
        for c in range(0, hidden, 256):
            h2[:count, c : c + 256] = silu_of_half(0.5 * dot(h1[:count, :], w2[:, c : c + 256])).astype(BF16)
        return dot(h2[:count, :], w3[...])

    def fill(base, pre, delta_t, k, groups):
        delta = jnp.transpose(delta_t)
        for g in groups:
            h1[base : base + rows, :] = silu_of_half(pre + delta[:, g : g + 1] * swapped[k, g : g + 1, :]).astype(BF16)
            base += rows
        return base

    row_in = lax.broadcasted_iota(jnp.int32, (window_rows, outputs), 0)

    def used(block):
        return jnp.concatenate(
            [(row_in + block * window_rows < ends[w]).astype(F32) for w in range(windows)], 0)

    def by_window(x):
        return jnp.sum(x.reshape(windows, window_rows, outputs), axis=1)

    def spread_rows(x):
        return jnp.concatenate(
            [jnp.broadcast_to(x[w : w + 1], (window_rows, outputs)) for w in range(windows)], 0)

    def count_of(block, w):
        count = jnp.minimum(jnp.maximum(ends[w] - block * window_rows, 0), window_rows)
        return jnp.full((1, outputs), count, jnp.int32).astype(F32)

    usable = used(me)
    st_copies, t_copies, b_copies = [], [], []
    out_a = None
    for index, ks in enumerate(near_plan(n)):
        base = 0
        for k in ks:
            base = fill(base, pre_a, d_send[partner(me, k, n)], k, range(gq))
        if index == 0:
            h1[base : base + 2 * rows, :] = silu_of_half(pre_ab).astype(BF16)
            base += 2 * rows
            loads[6].wait()
            loads[7].wait()
        out = tail(base)
        if index == 0:
            out_a = out[base - 2 * rows : base - rows]
            out_b = out[base - rows : base]
            counts = jnp.concatenate([count_of(me, w) for w in range(windows)], 0)
            inverse = 1.0 / jnp.maximum(counts, 1.0)
            mean = by_window(usable * (out_a + out_b)) * (0.5 * inverse)
            mean_rows = spread_rows(mean)
            dev_a = out_a - mean_rows
            dev_b = out_b - mean_rows
            shift = by_window(out_b) * (1.0 / window_rows)
            bt_send[:rows] = out_b
            stats = jnp.concatenate(
                [mean, by_window(usable * (dev_a * dev_a + dev_b * dev_b)), by_window(usable * out_b), shift], 0)
            bt_send[rows:] = stats
            t_near[0] = stats
            for i, (slot, peer) in enumerate(direct):
                b_copies.append(remote(bt_send, bt_far.at[slot], b_ss.at[i], b_rs.at[slot], {"rows": peer}))
                b_copies[-1].start()
            for k in range(1, half):
                t_copies.append(remote(bt_send.at[pl.ds(rows, 4 * windows)], t_near.at[k], t_ss.at[k], t_rs.at[k],
                                       {"rows": partner(me, k, n)}))
                t_copies[-1].start()
            shift_rows = spread_rows(shift)
            weighted_b = usable * (out_b - shift_rows)
        base = 0
        for k in ks:
            sums = [[], [], []]
            for g in range(gq):
                d = out[base : base + rows] - out_a
                base += rows
                masked = usable * d
                terms = (masked, masked * d, weighted_b * d)
                if k == 0:
                    for t in range(3):
                        acc[t, g] = terms[t]
                else:
                    for t in range(3):
                        sums[t].append(by_window(terms[t]))
            if k > 0:
                for t in range(3):
                    for w in range(windows):
                        st_send[k, t, w] = jnp.concatenate([x[w : w + 1] for x in sums[t]], 0)
                st_copies.append(remote(st_send.at[k], st_near.at[k], s_ss.at[k], s_rs.at[k],
                                        {"rows": partner(me, k, n)}))
                st_copies[-1].start()

    def wait_slot(buffer, rs, ss, slot):
        remote(buffer.at[slot], buffer.at[slot], ss, rs.at[slot], {"rows": me}).wait_recv()

    def far_fill(blocks, groups, fresh):
        base = 0
        for i, (slot, peer) in enumerate(blocks):
            if fresh:
                pre_s[i] = 0.5 * dot(a_far[slot].astype(BF16), w1[...])
            base = fill(base, pre_s[i], d_far[slot], 0, groups)
            if fresh:
                h1[base : base + rows, :] = silu_of_half(pre_s[i]).astype(BF16)
                base += rows
        return base

    def far_stats(blocks, groups, fresh, out):
        base = 0
        for i, (slot, peer) in enumerate(blocks):
            usable_k = used(peer)
            weighted = usable_k * (bt_far[slot, :rows] - shift_rows)
            if fresh:
                oa_s[i] = out[base + len(groups) * rows : base + (len(groups) + 1) * rows]
            out_ak = oa_s[i]
            for g in groups:
                d = out[base : base + rows] - out_ak
                base += rows
                masked = usable_k * d
                acc[0, g] += masked
                acc[1, g] += masked * d
                acc[2, g] += weighted * d
            if fresh:
                base += rows

    everything = list(range(gq))
    forwards = []
    for i, (slot, peer) in enumerate(first):
        wait_slot(a_far, a_rs, a_ss.at[0], slot)
        if share:
            forwards.append(remote(a_far.at[slot], a_far.at[slot], af_ss.at[i], a_rs.at[slot], mate))
            forwards[-1].start()
    for copy in d_copies:
        copy.wait_recv()
    out = tail(far_fill(first, everything, True))
    for i, (slot, peer) in enumerate(first):
        wait_slot(bt_far, b_rs, b_ss.at[0], slot)
        if share:
            forwards.append(remote(bt_far.at[slot], bt_far.at[slot], bf_ss.at[i], b_rs.at[slot], mate))
            forwards[-1].start()
    far_stats(first, everything, True, out)

    for slot, peer in second:
        wait_slot(a_far, a_rs, a_ss.at[0], slot)

    r_copies = []
    for stage in range(stages):
        groups = everything[stage * gh : (stage + 1) * gh]
        out = tail(far_fill(second, groups, stage == 0))
        if stage == 0:
            for slot, peer in second:
                wait_slot(bt_far, b_rs, b_ss.at[0], slot)
            for copy in t_copies + st_copies:
                copy.wait_recv()
            blocks = [(t_near[k], partner(me, k, n)) for k in range(half)]
            blocks += [(bt_far[slot, rows:], peer) for slot, peer in first + second]
            origin = t_near[0, 3 * windows : 3 * windows + 1]
            former = None
            finish = []
            for w in range(windows):
                count = [count_of(block, w) for _, block in blocks]
                now_n = sum(count)
                now_mean = sum(c * t[w : w + 1] for c, (t, _) in zip(count, blocks)) / now_n
                now_spread = sum(t[windows + w : windows + w + 1] for t, _ in blocks)
                now_spread += 2.0 * sum(c * jnp.square(t[w : w + 1] - now_mean)
                                        for c, (t, _) in zip(count, blocks))
                now_b = sum(t[2 * windows + w : 2 * windows + w + 1] for t, _ in blocks)
                if former is not None:
                    n1, m1, s1, b1 = former
                    both = n1 + now_n
                    change = now_mean - m1
                    share_n = now_n / both
                    now_spread = s1 + now_spread + 2.0 * change * change * n1 * share_n
                    now_mean = m1 + change * share_n
                    now_b = b1 + now_b
                    now_n = both
                former = (now_n, now_mean, now_spread, now_b)
                variance = now_spread / (2.0 * now_n)
                finish.append((1.0 / (now_n * variance), origin - now_b / now_n, variance))
        far_stats(second, groups, stage == 0, out)
        running = None
        for w in range(windows):
            local = [jnp.concatenate(
                [jnp.sum(acc[t, g, w * window_rows : (w + 1) * window_rows], axis=0, keepdims=True) for g in groups], 0)
                for t in range(3)]
            sum_d, sum_q = local[0], local[1]
            sum_x = local[2] + (t_near[0, 3 * windows + w : 3 * windows + w + 1] - origin) * sum_d
            for k in range(1, half):
                d_k = st_near[k, 0, w, stage * gh : (stage + 1) * gh]
                sum_x = sum_x + st_near[k, 2, w, stage * gh : (stage + 1) * gh]
                sum_x = sum_x + (t_near[k, 3 * windows + w : 3 * windows + w + 1] - origin) * d_k
                sum_q = sum_q + st_near[k, 1, w, stage * gh : (stage + 1) * gh]
                sum_d = sum_d + d_k
            now = (sum_d, sum_q, sum_x)
            running = now if running is None else tuple(x + y for x, y in zip(running, now))
            inverse_w, offset, _ = finish[w]
            res[me, stage, w, :gh] = (running[2] + offset * running[0]) * inverse_w
            res[me, stage, w, gh:] = 0.5 * running[1] * inverse_w
        for k in range(1, n):
            r_copies.append(remote(res.at[me, stage], res.at[me, stage], r_ss.at[stage, k], r_rs.at[stage, k],
                                   {"rows": partner(me, k, n)}))
            r_copies[-1].start()
    for w in range(windows):
        variance_ref[w : w + 1] = finish[w][2]
    for copy in r_copies:
        copy.wait_recv()
    for copy in a_copies + d_copies + b_copies + t_copies + st_copies + forwards + r_copies:
        copy.wait_send()


def deliver(n, res, variance_ref, first, total, variance):
    _, stages, windows, both, outputs = res.shape
    gh = both // 2
    for r in range(n):
        for w in range(windows):
            span = slice(r * stages * gh, (r + 1) * stages * gh)
            first[w, span] = jnp.concatenate([res[r, s, w, :gh] for s in range(stages)], 0)
            total[w, span] = jnp.concatenate([res[r, s, w, gh:] for s in range(stages)], 0)
    variance[...] = variance_ref[...]


def solution(mesh):
    n = mesh.shape["rows"]
    share = mesh.shape["par"] % 2 == 0

    def local(base_a, base_b, input_scale, layer_one, layer_two, layer_three, swap_cols, window_ends):
        windows, window_rows, width = base_a.shape
        groups = swap_cols.shape[0]
        gq = groups // n
        padded = -(-gq // 8) * 8
        stages = stage_count(gq)
        gh = gq // stages
        hidden = layer_two.shape[0]
        outputs = layer_three.shape[1]
        rows = windows * window_rows
        half, quarter = n // 2, n // 4
        most = max([(len(ks) * gq + 2 * (i == 0)) * rows for i, ks in enumerate(near_plan(n))]
                   + [quarter * (gq + 1) * rows])
        hbm = pl.BlockSpec(memory_space=pl.ANY)
        vmem = pl.BlockSpec(memory_space=pltpu.VMEM)
        dma = pltpu.SemaphoreType.DMA
        res, spread = pl.pallas_call(
            functools.partial(kernel, n, share),
            out_shape=(pltpu.VMEM((n, stages, windows, 2 * gh, outputs), F32), pltpu.VMEM((windows, outputs), F32)),
            in_specs=[hbm] * 8,
            out_specs=(vmem, vmem),
            scratch_shapes=[
                pltpu.VMEM(base_a.shape, BF16),
                pltpu.VMEM(base_b.shape, BF16),
                pltpu.VMEM((1, width), F32),
                pltpu.SMEM((groups,), jnp.int32),
                pltpu.SMEM((windows,), jnp.int32),
                pltpu.VMEM(layer_one.shape, BF16),
                pltpu.VMEM(layer_two.shape, BF16),
                pltpu.VMEM(layer_three.shape, BF16),
                pltpu.VMEM((rows, width), F32),
                pltpu.VMEM((half, rows, width), F32),
                pltpu.VMEM((n, padded, rows), F32),
                pltpu.VMEM((half, padded, rows), F32),
                pltpu.VMEM((n, padded, width), F32),
                pltpu.VMEM((half, padded, hidden), F32),
                pltpu.VMEM((rows + 4 * windows, outputs), F32),
                pltpu.VMEM((half, rows + 4 * windows, outputs), F32),
                pltpu.VMEM((half, 4 * windows, outputs), F32),
                pltpu.VMEM((half, 3, windows, gq, outputs), F32),
                pltpu.VMEM((half, 3, windows, gq, outputs), F32),
                pltpu.VMEM((3, gq, rows, outputs), F32),
                pltpu.VMEM((quarter, rows, hidden), F32),
                pltpu.VMEM((quarter, rows, outputs), F32),
                pltpu.VMEM((most, hidden), BF16),
                pltpu.VMEM((most, hidden), BF16),
                dma((8,)),
            ] + [dma((half,)) for _ in range(12)] + [dma((stages, n)) for _ in range(2)],
            compiler_params=pltpu.CompilerParams(
                collective_id=0, has_side_effects=True, vmem_limit_bytes=56 * 2**20
            ),
        )(base_a, base_b, input_scale.reshape(1, width), swap_cols, window_ends,
          layer_one, layer_two, layer_three)
        return pl.pallas_call(
            functools.partial(deliver, n),
            out_shape=(
                jax.ShapeDtypeStruct((windows, groups, outputs), F32),
                jax.ShapeDtypeStruct((windows, groups, outputs), F32),
                jax.ShapeDtypeStruct((windows, outputs), F32),
            ),
            in_specs=[vmem, vmem],
            out_specs=(vmem, vmem, vmem),
            compiler_params=pltpu.CompilerParams(vmem_limit_bytes=4 * 2**20),
        )(res, spread)

    in_specs = (P(None, "rows", None), P(None, "rows", None), P(), P(), P(), P(), P("par"), P())
    out_specs = (P(None, "par", None), P(None, "par", None), P())
    return jax.shard_map(local, mesh=mesh, in_specs=in_specs, out_specs=out_specs, check_vma=False)
```

```python
import functools

import jax
import jax.numpy as jnp
from jax import lax
from jax.experimental import pallas as pl
from jax.experimental.pallas import tpu as pltpu
from jax.sharding import PartitionSpec as P

F32 = jnp.float32
BF16 = jnp.bfloat16
MESH = pl.DeviceIdType.MESH


def silu_of_half(half):
    return half + half * jnp.tanh(half)


def dot(x, y):
    return jnp.dot(x, y, preferred_element_type=F32)


def dot_t(x, y):
    return lax.dot_general(x, y, (((1,), (1,)), ((), ())), preferred_element_type=F32)


def partner(me, k, n):
    other = me
    bit = 1
    while bit < n:
        if k & bit:
            other = other + bit - 2 * bit * lax.rem(other // bit, 2)
        bit *= 2
    return other


def near_plan(half):
    cut = half - max(1, half // 4)
    return list(range(half - 1, cut - 1, -1)), list(range(1, cut))


def stage_plan(count):
    last = max(1, count // 4)
    return [(0, count - last), (count - last, count)]


def kernel(n, a_hbm, b_hbm, scale_hbm, cols_hbm, ends_hbm, w1_hbm, w2_hbm, w3_hbm,
           res_0, res_1, variance_ref,
           base_a, base_b, scale, cols, ends, w1, w2, w3,
           a_send, a_near, d_send, d_near, onehot, swapped, b_send, b_near, t_all,
           st_send, st_near, acc, pre_s, oa_s, x_send_0, x_send_1, x_recv_0, x_recv_1, h1, h2,
           in_sems, a_ss, a_rs, d_ss, d_rs, b_ss, b_rs, s_ss, s_rs, t_ss, t_rs, x_ss, x_rs, r_ss, r_rs):
    windows, window_rows, width = base_a.shape
    padded = onehot.shape[2]
    hidden = w2.shape[0]
    outputs = w3.shape[1]
    rows = windows * window_rows
    half = n // 2
    gq = cols.shape[0] // n
    pg = 2 * gq
    by_sums, by_rows = near_plan(half)
    stages = stage_plan(pg)
    res, x_send, x_recv = (res_0, res_1), (x_send_0, x_send_1), (x_recv_0, x_recv_1)
    me = lax.axis_index("rows")
    kind = lax.rem(me, half)

    barrier = pltpu.get_barrier_semaphore()
    for k in range(1, n):
        pl.semaphore_signal(barrier, inc=1, device_id={"rows": partner(me, k, n)}, device_id_type=MESH)

    pairs = ((a_hbm, base_a), (b_hbm, base_b), (scale_hbm, scale), (cols_hbm, cols), (ends_hbm, ends),
             (w1_hbm, w1), (w2_hbm, w2), (w3_hbm, w3))
    loads = [pltpu.make_async_copy(src, dst, in_sems.at[i]) for i, (src, dst) in enumerate(pairs)]
    for load in loads:
        load.start()

    copies = []

    def send(src, dst, ss, rs, k):
        copy = pltpu.make_async_remote_copy(
            src_ref=src, dst_ref=dst, send_sem=ss, recv_sem=rs,
            device_id={"rows": partner(me, k, n)}, device_id_type=MESH)
        copy.start()
        copies.append(copy)
        return copy

    for load in loads[:5]:
        load.wait()
    factor = scale[...]
    own_a32 = (base_a[...].reshape(rows, width).astype(F32) * factor).astype(BF16).astype(F32)
    own_a = own_a32.astype(BF16)
    own_b = (base_b[...].reshape(rows, width).astype(F32) * factor).astype(BF16)
    a_send[...] = own_a32
    lane = lax.broadcasted_iota(jnp.int32, (padded, width), 1)
    sub = lax.broadcasted_iota(jnp.int32, (padded, width), 0)
    for r in range(n):
        wanted = jnp.full((padded, width), cols[r * gq], jnp.int32)
        for g in range(1, gq):
            wanted = jnp.where(sub == g, cols[r * gq + g], wanted)
        onehot[r % half, r // half] = (lane == wanted).astype(F32)
    marks = onehot[...].reshape(n * padded, width).astype(BF16)
    d_send[...] = (0.5 * (dot_t(marks, own_b) - dot_t(marks, own_a))).reshape(half, 2 * padded, rows)

    pl.semaphore_wait(barrier, n - 1)
    d_copies, a_copies = [], []
    for k in by_rows:
        d_copies.append(send(d_send.at[partner(kind, k, half)], d_near.at[k], d_ss.at[k], d_rs.at[k], k))
    for k in by_rows:
        a_copies.append(send(a_send, a_near.at[k], a_ss.at[k], a_rs.at[k], k))

    loads[5].wait()
    local = by_sums + [0]
    mark_near = jnp.concatenate(
        [onehot[partner(kind, k, half)].reshape(2 * padded, width) for k in local], 0).astype(BF16)
    swapped[...] = dot(mark_near, w1[...]).reshape(len(local), 2 * padded, hidden)
    pre_ab = 0.5 * dot(jnp.concatenate([own_a, own_b], 0), w1[...])
    pre_a = pre_ab[:rows]

    def tail(count):
        for c in range(0, hidden, 256):
            h2[:count, c : c + 256] = silu_of_half(0.5 * dot(h1[:count, :], w2[:, c : c + 256])).astype(BF16)
        return dot(h2[:count, :], w3[...])

    def fill(base, pre, delta_t, i, groups):
        delta = jnp.transpose(delta_t)
        for g in groups:
            at = (g // gq) * padded + g % gq
            h1[base : base + rows, :] = silu_of_half(
                pre + delta[:, at : at + 1] * swapped[i, at : at + 1, :]).astype(BF16)
            base += rows
        return base

    row_in = lax.broadcasted_iota(jnp.int32, (window_rows, outputs), 0)

    def used(block):
        return jnp.concatenate(
            [(row_in + block * window_rows < ends[w]).astype(F32) for w in range(windows)], 0)

    def by_window(x):
        return jnp.sum(x.reshape(windows, window_rows, outputs), axis=1)

    def spread_rows(x):
        return jnp.concatenate(
            [jnp.broadcast_to(x[w : w + 1], (window_rows, outputs)) for w in range(windows)], 0)

    def count_of(block, w):
        count = jnp.minimum(jnp.maximum(ends[w] - block * window_rows, 0), window_rows)
        return jnp.full((1, outputs), count, jnp.int32).astype(F32)

    everything = range(pg)
    usable = used(me)

    base = 0
    for i, k in enumerate(by_sums):
        base = fill(base, pre_a, d_send[partner(kind, k, half)], i, everything)
    h1[base : base + 2 * rows, :] = silu_of_half(pre_ab).astype(BF16)
    loads[6].wait()
    loads[7].wait()
    out = tail(base + 2 * rows)
    out_a = out[base : base + rows]
    out_b = out[base + rows : base + 2 * rows]
    b_send[...] = out_b
    b_copies = [send(b_send, b_near.at[k], b_ss.at[k], b_rs.at[k], k) for k in by_rows]
    counts = jnp.concatenate([count_of(me, w) for w in range(windows)], 0)
    mean = by_window(usable * (out_a + out_b)) * (0.5 / jnp.maximum(counts, 1.0))
    mean_rows = spread_rows(mean)
    dev_a = out_a - mean_rows
    dev_b = out_b - mean_rows
    shift = by_window(out_b) * (1.0 / window_rows)
    t_all[0] = jnp.concatenate(
        [mean, by_window(usable * (dev_a * dev_a + dev_b * dev_b)), by_window(usable * out_b), shift], 0)
    t_copies = [send(t_all.at[0], t_all.at[k], t_ss.at[k], t_rs.at[k], k) for k in range(n - 1, 0, -1)]
    shift_rows = spread_rows(shift)
    weighted_b = usable * (out_b - shift_rows)
    base = 0
    s_copies = []
    for k in by_sums:
        sums = [[], [], []]
        for g in everything:
            d = out[base : base + rows] - out_a
            base += rows
            masked = usable * d
            for t, term in enumerate((masked, masked * d, weighted_b * d)):
                sums[t].append(by_window(term))
        for t in range(3):
            for w in range(windows):
                st_send[k, t, w] = jnp.concatenate([x[w : w + 1] for x in sums[t]], 0)
        s_copies.append(send(st_send.at[k], st_near.at[k], s_ss.at[k], s_rs.at[k], k))

    out = tail(fill(0, pre_a, d_send[kind], len(by_sums), everything))
    for g in everything:
        d = out[g * rows : (g + 1) * rows] - out_a
        masked = usable * d
        acc[0, g] = masked
        acc[1, g] = masked * d
        acc[2, g] = weighted_b * d

    for copy in d_copies + a_copies:
        copy.wait_recv()

    x_copies = []
    for stage, (start, stop) in enumerate(stages):
        groups = range(start, stop)
        base = 0
        for i, k in enumerate(by_rows):
            if stage == 0:
                pre_s[i] = 0.5 * dot(a_near[k].astype(BF16), w1[...])
            base = fill(base, pre_s[i], d_near[k], len(by_sums), groups)
            if stage == 0:
                h1[base : base + rows, :] = silu_of_half(pre_s[i]).astype(BF16)
                base += rows
        out = tail(base)
        if stage == 0:
            for copy in b_copies:
                copy.wait_recv()
        base = 0
        for i, k in enumerate(by_rows):
            usable_k = used(partner(me, k, n))
            weighted = usable_k * (b_near[k] - shift_rows)
            if stage == 0:
                oa_s[i] = out[base + len(groups) * rows : base + (len(groups) + 1) * rows]
            out_ak = oa_s[i]
            for g in groups:
                d = out[base : base + rows] - out_ak
                base += rows
                masked = usable_k * d
                acc[0, g] += masked
                acc[1, g] += masked * d
                acc[2, g] += weighted * d
            if stage == 0:
                base += rows
        if stage == 0:
            for copy in t_copies + s_copies:
                copy.wait_recv()
            origin = t_all[0, 3 * windows : 3 * windows + 1]
            blocks = [partner(me, k, n) for k in range(n)]
            former = None
            finish = []
            for w in range(windows):
                count = [count_of(block, w) for block in blocks]
                now_n = sum(count)
                now_mean = sum(c * t_all[k, w : w + 1] for k, c in enumerate(count)) / now_n
                now_spread = sum(t_all[k, windows + w : windows + w + 1] for k in range(n))
                now_spread += 2.0 * sum(c * jnp.square(t_all[k, w : w + 1] - now_mean) for k, c in enumerate(count))
                now_b = sum(t_all[k, 2 * windows + w : 2 * windows + w + 1] for k in range(n))
                if former is not None:
                    n1, m1, s1, b1 = former
                    both = n1 + now_n
                    change = now_mean - m1
                    part = now_n / both
                    now_spread = s1 + now_spread + 2.0 * change * change * n1 * part
                    now_mean = m1 + change * part
                    now_b = b1 + now_b
                    now_n = both
                former = (now_n, now_mean, now_spread, now_b)
                variance = now_spread / (2.0 * now_n)
                variance_ref[w : w + 1] = variance
                finish.append((1.0 / (now_n * variance), now_b / now_n))
        running = None
        for w in range(windows):
            sum_d, sum_q, sum_x = [jnp.concatenate(
                [jnp.sum(acc[t, g, w * window_rows : (w + 1) * window_rows], axis=0, keepdims=True) for g in groups], 0)
                for t in range(3)]
            sum_x = sum_x + (t_all[0, 3 * windows + w : 3 * windows + w + 1] - origin) * sum_d
            for k in by_sums:
                d_k = st_near[k, 0, w, start:stop]
                sum_x = sum_x + st_near[k, 2, w, start:stop]
                sum_x = sum_x + (t_all[k, 3 * windows + w : 3 * windows + w + 1] - origin) * d_k
                sum_q = sum_q + st_near[k, 1, w, start:stop]
                sum_d = sum_d + d_k
            now = (sum_d, sum_q, sum_x)
            running = now if running is None else tuple(x + y for x, y in zip(running, now))
            x_send[stage][w, : stop - start] = running[2] + (origin - finish[w][1]) * running[0]
            x_send[stage][w, stop - start :] = 0.5 * running[1]
        x_copies.append(send(x_send[stage], x_recv[stage], x_ss.at[stage], x_rs.at[stage], half))

    r_copies = []
    for stage in range(2):
        x_copies[stage].wait_recv()
        for w in range(windows):
            res[stage][kind, w] = (x_send[stage][w] + x_recv[stage][w]) * finish[w][0]
        for k in range(half - 1, 0, -1):
            mine = res[stage].at[kind]
            r_copies.append(send(mine, mine, r_ss.at[stage, k], r_rs.at[stage, k], k))
    for copy in r_copies:
        copy.wait_recv()
    for copy in copies:
        copy.wait_send()


def deliver(gq, res_0, res_1, variance_ref, first, total, variance):
    half, windows = res_0.shape[:2]
    cut, rest = res_0.shape[2] // 2, res_1.shape[2] // 2
    for kind in range(half):
        for w in range(windows):
            for out, early, late in ((first, res_0[kind, w, :cut], res_1[kind, w, :rest]),
                                     (total, res_0[kind, w, cut:], res_1[kind, w, rest:])):
                both = jnp.concatenate([early, late], 0)
                out[w, kind * gq : (kind + 1) * gq] = both[:gq]
                out[w, (half + kind) * gq : (half + kind + 1) * gq] = both[gq:]
    variance[...] = variance_ref[...]


def solution(mesh):
    n = mesh.shape["rows"]

    def local(base_a, base_b, input_scale, layer_one, layer_two, layer_three, swap_cols, window_ends):
        windows, window_rows, width = base_a.shape
        groups = swap_cols.shape[0]
        gq = groups // n
        pg = 2 * gq
        padded = -(-gq // 8) * 8
        hidden = layer_two.shape[0]
        outputs = layer_three.shape[1]
        rows = windows * window_rows
        half = n // 2
        by_sums, by_rows = near_plan(half)
        sizes = [2 * (stop - start) for start, stop in stage_plan(pg)]
        most = rows * max(len(by_sums) * pg + 2, pg, len(by_rows) * (sizes[0] // 2 + 1), len(by_rows) * sizes[1] // 2)
        hbm = pl.BlockSpec(memory_space=pl.ANY)
        vmem = pl.BlockSpec(memory_space=pltpu.VMEM)
        dma = pltpu.SemaphoreType.DMA
        results = pl.pallas_call(
            functools.partial(kernel, n),
            out_shape=tuple(pltpu.VMEM((half, windows, size, outputs), F32) for size in sizes)
            + (pltpu.VMEM((windows, outputs), F32),),
            in_specs=[hbm] * 8,
            out_specs=(vmem,) * 3,
            scratch_shapes=[
                pltpu.VMEM(base_a.shape, BF16),
                pltpu.VMEM(base_b.shape, BF16),
                pltpu.VMEM((1, width), F32),
                pltpu.SMEM((groups,), jnp.int32),
                pltpu.SMEM((windows,), jnp.int32),
                pltpu.VMEM(layer_one.shape, BF16),
                pltpu.VMEM(layer_two.shape, BF16),
                pltpu.VMEM(layer_three.shape, BF16),
                pltpu.VMEM((rows, width), F32),
                pltpu.VMEM((half, rows, width), F32),
                pltpu.VMEM((half, 2 * padded, rows), F32),
                pltpu.VMEM((half, 2 * padded, rows), F32),
                pltpu.VMEM((half, 2, padded, width), F32),
                pltpu.VMEM((len(by_sums) + 1, 2 * padded, hidden), F32),
                pltpu.VMEM((rows, outputs), F32),
                pltpu.VMEM((half, rows, outputs), F32),
                pltpu.VMEM((n, 4 * windows, outputs), F32),
                pltpu.VMEM((half, 3, windows, pg, outputs), F32),
                pltpu.VMEM((half, 3, windows, pg, outputs), F32),
                pltpu.VMEM((3, pg, rows, outputs), F32),
                pltpu.VMEM((len(by_rows), rows, hidden), F32),
                pltpu.VMEM((len(by_rows), rows, outputs), F32),
            ] + [pltpu.VMEM((windows, size, outputs), F32) for size in sizes + sizes] + [
                pltpu.VMEM((most, hidden), BF16),
                pltpu.VMEM((most, hidden), BF16),
                dma((8,)),
            ] + [dma((half,)) for _ in range(8)] + [dma((n,)), dma((n,)), dma((2,)), dma((2,)),
                                                    dma((2, half)), dma((2, half))],
            compiler_params=pltpu.CompilerParams(
                collective_id=0, has_side_effects=True, vmem_limit_bytes=56 * 2**20
            ),
        )(base_a, base_b, input_scale.reshape(1, width), swap_cols, window_ends,
          layer_one, layer_two, layer_three)
        return pl.pallas_call(
            functools.partial(deliver, gq),
            out_shape=(
                jax.ShapeDtypeStruct((windows, groups, outputs), F32),
                jax.ShapeDtypeStruct((windows, groups, outputs), F32),
                jax.ShapeDtypeStruct((windows, outputs), F32),
            ),
            in_specs=[vmem] * 3,
            out_specs=(vmem, vmem, vmem),
            compiler_params=pltpu.CompilerParams(vmem_limit_bytes=4 * 2**20),
        )(*results)

    in_specs = (P(None, "rows", None), P(None, "rows", None), P(), P(), P(), P(), P("par"), P())
    out_specs = (P(None, "par", None), P(None, "par", None), P())
    return jax.shard_map(local, mesh=mesh, in_specs=in_specs, out_specs=out_specs, check_vma=False)
```

```python
import functools

import jax
import jax.numpy as jnp
from jax import lax
from jax.experimental import pallas as pl
from jax.experimental.pallas import tpu as pltpu
from jax.sharding import PartitionSpec as P

F32 = jnp.float32
BF16 = jnp.bfloat16
MESH = pl.DeviceIdType.MESH


def silu_of_half(half):
    return half + half * jnp.tanh(half)


def dot(x, y):
    return jnp.dot(x, y, preferred_element_type=F32)


def dot_t(x, y):
    return lax.dot_general(x, y, (((1,), (1,)), ((), ())), preferred_element_type=F32)


def partner(me, k, n):
    other = me
    bit = 1
    while bit < n:
        if k & bit:
            other = other + bit - 2 * bit * lax.rem(other // bit, 2)
        bit *= 2
    return other


def near_plan(half):
    cut = half - max(1, half // 4)
    return list(range(half - 1, cut - 1, -1)), list(range(1, cut))


def stage_plan(count):
    last = max(1, count // 4)
    return [(0, count - last), (count - last, count)]


def kernel(n, a_hbm, b_hbm, scale_hbm, cols_hbm, ends_hbm, w1_hbm, w2_hbm, w3_hbm,
           res_0, res_1, variance_ref,
           base_a, base_b, scale, cols, ends, w1, w2, w3,
           a_send, a_near, d_send, d_near, onehot, swapped, b_send, b_near, t_all,
           st_send, st_near, acc, pre_s, oa_s, x_send_0, x_send_1, x_recv_0, x_recv_1, h1, h2,
           in_sems, a_ss, a_rs, d_ss, d_rs, b_ss, b_rs, s_ss, s_rs, t_ss, t_rs, x_ss, x_rs, r_ss, r_rs):
    windows, window_rows, width = base_a.shape
    padded = onehot.shape[2]
    hidden = w2.shape[0]
    outputs = w3.shape[1]
    rows = windows * window_rows
    half = n // 2
    gq = cols.shape[0] // n
    pg = 2 * gq
    by_sums, by_rows = near_plan(half)
    stages = stage_plan(pg)
    res, x_send, x_recv = (res_0, res_1), (x_send_0, x_send_1), (x_recv_0, x_recv_1)
    me = lax.axis_index("rows")
    kind = lax.rem(me, half)

    barrier = pltpu.get_barrier_semaphore()
    for k in range(1, n):
        pl.semaphore_signal(barrier, inc=1, device_id={"rows": partner(me, k, n)}, device_id_type=MESH)

    pairs = ((a_hbm, base_a), (b_hbm, base_b), (scale_hbm, scale), (cols_hbm, cols), (ends_hbm, ends),
             (w1_hbm, w1), (w2_hbm, w2), (w3_hbm, w3))
    loads = [pltpu.make_async_copy(src, dst, in_sems.at[i]) for i, (src, dst) in enumerate(pairs)]
    for load in loads:
        load.start()

    copies = []

    def send(src, dst, ss, rs, k):
        copy = pltpu.make_async_remote_copy(
            src_ref=src, dst_ref=dst, send_sem=ss, recv_sem=rs,
            device_id={"rows": partner(me, k, n)}, device_id_type=MESH)
        copy.start()
        copies.append(copy)
        return copy

    for load in loads[:5]:
        load.wait()
    factor = scale[...]
    own_a32 = (base_a[...].reshape(rows, width).astype(F32) * factor).astype(BF16).astype(F32)
    own_a = own_a32.astype(BF16)
    own_b = (base_b[...].reshape(rows, width).astype(F32) * factor).astype(BF16)
    a_send[...] = own_a32
    lane = lax.broadcasted_iota(jnp.int32, (padded, width), 1)
    sub = lax.broadcasted_iota(jnp.int32, (padded, width), 0)
    for r in range(n):
        wanted = jnp.full((padded, width), cols[r * gq], jnp.int32)
        for g in range(1, gq):
            wanted = jnp.where(sub == g, cols[r * gq + g], wanted)
        onehot[r % half, r // half] = (lane == wanted).astype(F32)
    marks = onehot[...].reshape(n * padded, width).astype(BF16)
    d_send[...] = (0.5 * (dot_t(marks, own_b) - dot_t(marks, own_a))).reshape(half, 2 * padded, rows)

    pl.semaphore_wait(barrier, n - 1)
    d_copies, a_copies = [], []
    for k in by_rows:
        d_copies.append(send(d_send.at[partner(kind, k, half)], d_near.at[k], d_ss.at[k], d_rs.at[k], k))
    for k in by_rows:
        a_copies.append(send(a_send, a_near.at[k], a_ss.at[k], a_rs.at[k], k))

    loads[5].wait()
    local = by_sums + [0]
    mark_near = jnp.concatenate(
        [onehot[partner(kind, k, half)].reshape(2 * padded, width) for k in local], 0).astype(BF16)
    swapped[...] = dot(mark_near, w1[...]).reshape(len(local), 2 * padded, hidden)
    pre_ab = 0.5 * dot(jnp.concatenate([own_a, own_b], 0), w1[...])
    pre_a = pre_ab[:rows]

    def tail(count):
        for c in range(0, hidden, 256):
            h2[:count, c : c + 256] = silu_of_half(0.5 * dot(h1[:count, :], w2[:, c : c + 256])).astype(BF16)
        mid = count // 2 // 16 * 16
        return jnp.concatenate([dot(h2[:mid, :], w3[...]), dot(h2[mid:count, :], w3[...])], 0)

    def fill(base, pre, delta_t, i, groups):
        delta = jnp.transpose(delta_t)
        for g in groups:
            at = (g // gq) * padded + g % gq
            h1[base : base + rows, :] = silu_of_half(
                pre + delta[:, at : at + 1] * swapped[i, at : at + 1, :]).astype(BF16)
            base += rows
        return base

    row_in = lax.broadcasted_iota(jnp.int32, (window_rows, outputs), 0)

    def used(block):
        return jnp.concatenate(
            [(row_in + block * window_rows < ends[w]).astype(F32) for w in range(windows)], 0)

    def by_window(x):
        return jnp.sum(x.reshape(windows, window_rows, outputs), axis=1)

    def spread_rows(x):
        return jnp.concatenate(
            [jnp.broadcast_to(x[w : w + 1], (window_rows, outputs)) for w in range(windows)], 0)

    def count_of(block, w):
        count = jnp.minimum(jnp.maximum(ends[w] - block * window_rows, 0), window_rows)
        return jnp.full((1, outputs), count, jnp.int32).astype(F32)

    everything = range(pg)
    usable = used(me)

    loads[6].wait()
    loads[7].wait()
    base = 0
    for i, k in enumerate(by_sums):
        base = fill(base, pre_a, d_send[partner(kind, k, half)], i, everything)
    h1[base : base + 2 * rows, :] = silu_of_half(pre_ab).astype(BF16)
    out = tail(base + 2 * rows)
    out_a = out[base : base + rows]
    out_b = out[base + rows : base + 2 * rows]
    b_send[...] = out_b
    b_copies = [send(b_send, b_near.at[k], b_ss.at[k], b_rs.at[k], k) for k in by_rows]
    counts = jnp.concatenate([count_of(me, w) for w in range(windows)], 0)
    mean = by_window(usable * (out_a + out_b)) * (0.5 / jnp.maximum(counts, 1.0))
    mean_rows = spread_rows(mean)
    dev_a = out_a - mean_rows
    dev_b = out_b - mean_rows
    shift = by_window(out_b) * (1.0 / window_rows)
    t_all[0] = jnp.concatenate(
        [mean, by_window(usable * (dev_a * dev_a + dev_b * dev_b)), by_window(usable * out_b), shift], 0)
    t_copies = [send(t_all.at[0], t_all.at[k], t_ss.at[k], t_rs.at[k], k) for k in range(n - 1, 0, -1)]
    shift_rows = spread_rows(shift)
    weighted_b = usable * (out_b - shift_rows)
    base = 0
    s_copies = []
    for k in by_sums:
        sums = [[], [], []]
        for g in everything:
            d = out[base : base + rows] - out_a
            base += rows
            masked = usable * d
            for t, term in enumerate((masked, masked * d, weighted_b * d)):
                sums[t].append(by_window(term))
        for t in range(3):
            for w in range(windows):
                st_send[k, t, w] = jnp.concatenate([x[w : w + 1] for x in sums[t]], 0)
        s_copies.append(send(st_send.at[k], st_near.at[k], s_ss.at[k], s_rs.at[k], k))

    out = tail(fill(0, pre_a, d_send[kind], len(by_sums), everything))
    for g in everything:
        d = out[g * rows : (g + 1) * rows] - out_a
        masked = usable * d
        acc[0, g] = masked
        acc[1, g] = masked * d
        acc[2, g] = weighted_b * d

    for copy in d_copies + a_copies:
        copy.wait_recv()

    x_copies = []
    for stage, (start, stop) in enumerate(stages):
        groups = range(start, stop)
        base = 0
        for i, k in enumerate(by_rows):
            if stage == 0:
                pre_s[i] = 0.5 * dot(a_near[k].astype(BF16), w1[...])
            base = fill(base, pre_s[i], d_near[k], len(by_sums), groups)
            if stage == 0:
                h1[base : base + rows, :] = silu_of_half(pre_s[i]).astype(BF16)
                base += rows
        out = tail(base)
        if stage == 0:
            for copy in b_copies:
                copy.wait_recv()
        base = 0
        for i, k in enumerate(by_rows):
            usable_k = used(partner(me, k, n))
            weighted = usable_k * (b_near[k] - shift_rows)
            if stage == 0:
                oa_s[i] = out[base + len(groups) * rows : base + (len(groups) + 1) * rows]
            out_ak = oa_s[i]
            for g in groups:
                d = out[base : base + rows] - out_ak
                base += rows
                masked = usable_k * d
                acc[0, g] += masked
                acc[1, g] += masked * d
                acc[2, g] += weighted * d
            if stage == 0:
                base += rows
        if stage == 0:
            for copy in t_copies + s_copies:
                copy.wait_recv()
            origin = t_all[0, 3 * windows : 3 * windows + 1]
            blocks = [partner(me, k, n) for k in range(n)]
            former = None
            finish = []
            for w in range(windows):
                count = [count_of(block, w) for block in blocks]
                now_n = sum(count)
                now_mean = sum(c * t_all[k, w : w + 1] for k, c in enumerate(count)) / now_n
                now_spread = sum(t_all[k, windows + w : windows + w + 1] for k in range(n))
                now_spread += 2.0 * sum(c * jnp.square(t_all[k, w : w + 1] - now_mean) for k, c in enumerate(count))
                now_b = sum(t_all[k, 2 * windows + w : 2 * windows + w + 1] for k in range(n))
                if former is not None:
                    n1, m1, s1, b1 = former
                    both = n1 + now_n
                    change = now_mean - m1
                    part = now_n / both
                    now_spread = s1 + now_spread + 2.0 * change * change * n1 * part
                    now_mean = m1 + change * part
                    now_b = b1 + now_b
                    now_n = both
                former = (now_n, now_mean, now_spread, now_b)
                variance = now_spread / (2.0 * now_n)
                variance_ref[w : w + 1] = variance
                finish.append((1.0 / (now_n * variance), now_b / now_n))
        running = None
        for w in range(windows):
            sum_d, sum_q, sum_x = [jnp.concatenate(
                [jnp.sum(acc[t, g, w * window_rows : (w + 1) * window_rows], axis=0, keepdims=True) for g in groups], 0)
                for t in range(3)]
            sum_x = sum_x + (t_all[0, 3 * windows + w : 3 * windows + w + 1] - origin) * sum_d
            for k in by_sums:
                d_k = st_near[k, 0, w, start:stop]
                sum_x = sum_x + st_near[k, 2, w, start:stop]
                sum_x = sum_x + (t_all[k, 3 * windows + w : 3 * windows + w + 1] - origin) * d_k
                sum_q = sum_q + st_near[k, 1, w, start:stop]
                sum_d = sum_d + d_k
            now = (sum_d, sum_q, sum_x)
            running = now if running is None else tuple(x + y for x, y in zip(running, now))
            x_send[stage][w, : stop - start] = running[2] + (origin - finish[w][1]) * running[0]
            x_send[stage][w, stop - start :] = 0.5 * running[1]
        x_copies.append(send(x_send[stage], x_recv[stage], x_ss.at[stage], x_rs.at[stage], half))

    r_copies = []
    for stage in range(2):
        x_copies[stage].wait_recv()
        for w in range(windows):
            res[stage][kind, w] = (x_send[stage][w] + x_recv[stage][w]) * finish[w][0]
        for k in range(half - 1, 0, -1):
            mine = res[stage].at[kind]
            r_copies.append(send(mine, mine, r_ss.at[stage, k], r_rs.at[stage, k], k))
    for copy in r_copies:
        copy.wait_recv()
    for copy in copies:
        copy.wait_send()


def deliver(gq, res_0, res_1, variance_ref, first, total, variance):
    half, windows = res_0.shape[:2]
    cut, rest = res_0.shape[2] // 2, res_1.shape[2] // 2
    for kind in range(half):
        for w in range(windows):
            for out, early, late in ((first, res_0[kind, w, :cut], res_1[kind, w, :rest]),
                                     (total, res_0[kind, w, cut:], res_1[kind, w, rest:])):
                both = jnp.concatenate([early, late], 0)
                out[w, kind * gq : (kind + 1) * gq] = both[:gq]
                out[w, (half + kind) * gq : (half + kind + 1) * gq] = both[gq:]
    variance[...] = variance_ref[...]


def solution(mesh):
    n = mesh.shape["rows"]

    def local(base_a, base_b, input_scale, layer_one, layer_two, layer_three, swap_cols, window_ends):
        windows, window_rows, width = base_a.shape
        groups = swap_cols.shape[0]
        gq = groups // n
        pg = 2 * gq
        padded = -(-gq // 8) * 8
        hidden = layer_two.shape[0]
        outputs = layer_three.shape[1]
        rows = windows * window_rows
        half = n // 2
        by_sums, by_rows = near_plan(half)
        sizes = [2 * (stop - start) for start, stop in stage_plan(pg)]
        most = rows * max(len(by_sums) * pg + 2, pg, len(by_rows) * (sizes[0] // 2 + 1), len(by_rows) * sizes[1] // 2)
        hbm = pl.BlockSpec(memory_space=pl.ANY)
        vmem = pl.BlockSpec(memory_space=pltpu.VMEM)
        dma = pltpu.SemaphoreType.DMA
        results = pl.pallas_call(
            functools.partial(kernel, n),
            out_shape=tuple(pltpu.VMEM((half, windows, size, outputs), F32) for size in sizes)
            + (pltpu.VMEM((windows, outputs), F32),),
            in_specs=[hbm] * 8,
            out_specs=(vmem,) * 3,
            scratch_shapes=[
                pltpu.VMEM(base_a.shape, BF16),
                pltpu.VMEM(base_b.shape, BF16),
                pltpu.VMEM((1, width), F32),
                pltpu.SMEM((groups,), jnp.int32),
                pltpu.SMEM((windows,), jnp.int32),
                pltpu.VMEM(layer_one.shape, BF16),
                pltpu.VMEM(layer_two.shape, BF16),
                pltpu.VMEM(layer_three.shape, BF16),
                pltpu.VMEM((rows, width), F32),
                pltpu.VMEM((half, rows, width), F32),
                pltpu.VMEM((half, 2 * padded, rows), F32),
                pltpu.VMEM((half, 2 * padded, rows), F32),
                pltpu.VMEM((half, 2, padded, width), F32),
                pltpu.VMEM((len(by_sums) + 1, 2 * padded, hidden), F32),
                pltpu.VMEM((rows, outputs), F32),
                pltpu.VMEM((half, rows, outputs), F32),
                pltpu.VMEM((n, 4 * windows, outputs), F32),
                pltpu.VMEM((half, 3, windows, pg, outputs), F32),
                pltpu.VMEM((half, 3, windows, pg, outputs), F32),
                pltpu.VMEM((3, pg, rows, outputs), F32),
                pltpu.VMEM((len(by_rows), rows, hidden), F32),
                pltpu.VMEM((len(by_rows), rows, outputs), F32),
            ] + [pltpu.VMEM((windows, size, outputs), F32) for size in sizes + sizes] + [
                pltpu.VMEM((most, hidden), BF16),
                pltpu.VMEM((most, hidden), BF16),
                dma((8,)),
            ] + [dma((half,)) for _ in range(8)] + [dma((n,)), dma((n,)), dma((2,)), dma((2,)),
                                                    dma((2, half)), dma((2, half))],
            compiler_params=pltpu.CompilerParams(
                collective_id=0, has_side_effects=True, vmem_limit_bytes=56 * 2**20
            ),
        )(base_a, base_b, input_scale.reshape(1, width), swap_cols, window_ends,
          layer_one, layer_two, layer_three)
        return pl.pallas_call(
            functools.partial(deliver, gq),
            out_shape=(
                jax.ShapeDtypeStruct((windows, groups, outputs), F32),
                jax.ShapeDtypeStruct((windows, groups, outputs), F32),
                jax.ShapeDtypeStruct((windows, outputs), F32),
            ),
            in_specs=[vmem] * 3,
            out_specs=(vmem, vmem, vmem),
            compiler_params=pltpu.CompilerParams(vmem_limit_bytes=4 * 2**20),
        )(*results)

    in_specs = (P(None, "rows", None), P(None, "rows", None), P(), P(), P(), P(), P("par"), P())
    out_specs = (P(None, "par", None), P(None, "par", None), P())
    return jax.shard_map(local, mesh=mesh, in_specs=in_specs, out_specs=out_specs, check_vma=False)
```

```python
import functools

import jax
import jax.numpy as jnp
from jax import lax
from jax.experimental import pallas as pl
from jax.experimental.pallas import tpu as pltpu
from jax.sharding import PartitionSpec as P

F32 = jnp.float32
BF16 = jnp.bfloat16
MESH = pl.DeviceIdType.MESH


def silu_of_half(half):
    return half + half * jnp.tanh(half)


def dot(x, y):
    return jnp.dot(x, y, preferred_element_type=F32)


def dot_t(x, y):
    return lax.dot_general(x, y, (((1,), (1,)), ((), ())), preferred_element_type=F32)


def partner(me, k, n):
    other = me
    bit = 1
    while bit < n:
        if k & bit:
            other = other + bit - 2 * bit * lax.rem(other // bit, 2)
        bit *= 2
    return other


def near_plan(half):
    cut = half - max(1, half // 4)
    return list(range(half - 1, cut - 1, -1)), list(range(1, cut))


def part_size(count):
    return max(1, count // 4)


def fold(parts):
    row = lax.broadcasted_iota(jnp.int32, parts[0].shape, 0)
    for bit in (4, 2, 1):
        low = (row // bit) % 2 == 0
        merged = []
        for a, b in zip(parts[: len(parts) // 2], parts[len(parts) // 2 :]):
            if bit == 4:
                merged.append(jnp.where(low, a, b) + pltpu.roll(jnp.where(low, b, a), 4, 0))
            else:
                merged.append(jnp.where(low, a + pltpu.roll(a, 8 - bit, 0), b + pltpu.roll(b, bit, 0)))
        parts = merged
    return parts[0]


def sum_each(parts):
    if parts[0].shape[0] != 8 or len(parts) % 8:
        return jnp.concatenate([jnp.sum(x, axis=0, keepdims=True) for x in parts], 0)
    return jnp.concatenate([fold(parts[i : i + 8]) for i in range(0, len(parts), 8)], 0)


def kernel(n, a_hbm, b_hbm, scale_hbm, cols_hbm, ends_hbm, w1_hbm, w2_hbm, w3_hbm,
           res, variance_ref,
           base_a, base_b, scale, cols, ends, w1, w2, w3,
           a_send, a_near, d_send, d_near, onehot, swapped, b_send, b_near, t_all,
           st_send, st_near, acc, pre_s, oa_s, x_send, x_recv, h1, h2,
           in_sems, a_ss, a_rs, d_ss, d_rs, b_ss, b_rs, s_ss, s_rs, t_ss, t_rs, x_ss, x_rs, r_ss, r_rs):
    windows, window_rows, width = base_a.shape
    padded = onehot.shape[2]
    hidden = w2.shape[0]
    outputs = w3.shape[1]
    rows = windows * window_rows
    half = n // 2
    gq = cols.shape[0] // n
    pg = 2 * gq
    by_sums, by_rows = near_plan(half)
    gp = part_size(pg)
    parts = pg // gp
    stages = [(0, parts - 1), (parts - 1, parts)]
    me = lax.axis_index("rows")
    kind = lax.rem(me, half)

    barrier = pltpu.get_barrier_semaphore()
    for k in range(1, n):
        pl.semaphore_signal(barrier, inc=1, device_id={"rows": partner(me, k, n)}, device_id_type=MESH)

    pairs = ((a_hbm, base_a), (b_hbm, base_b), (scale_hbm, scale), (cols_hbm, cols), (ends_hbm, ends),
             (w1_hbm, w1), (w2_hbm, w2), (w3_hbm, w3))
    loads = [pltpu.make_async_copy(src, dst, in_sems.at[i]) for i, (src, dst) in enumerate(pairs)]
    for load in loads:
        load.start()

    copies = []

    def send(src, dst, ss, rs, k):
        copy = pltpu.make_async_remote_copy(
            src_ref=src, dst_ref=dst, send_sem=ss, recv_sem=rs,
            device_id={"rows": partner(me, k, n)}, device_id_type=MESH)
        copy.start()
        copies.append(copy)
        return copy

    for load in loads[:5]:
        load.wait()
    factor = scale[...]
    own_a32 = (base_a[...].reshape(rows, width).astype(F32) * factor).astype(BF16).astype(F32)
    own_a = own_a32.astype(BF16)
    own_b = (base_b[...].reshape(rows, width).astype(F32) * factor).astype(BF16)
    a_send[...] = own_a32
    lane = lax.broadcasted_iota(jnp.int32, (padded, width), 1)
    sub = lax.broadcasted_iota(jnp.int32, (padded, width), 0)
    for r in range(n):
        wanted = jnp.full((padded, width), cols[r * gq], jnp.int32)
        for g in range(1, gq):
            wanted = jnp.where(sub == g, cols[r * gq + g], wanted)
        onehot[r % half, r // half] = (lane == wanted).astype(F32)
    marks = onehot[...].reshape(n * padded, width).astype(BF16)
    d_send[...] = (0.5 * (dot_t(marks, own_b) - dot_t(marks, own_a))).reshape(half, 2 * padded, rows)

    pl.semaphore_wait(barrier, n - 1)
    d_copies, a_copies = [], []
    for k in by_rows:
        d_copies.append(send(d_send.at[partner(kind, k, half)], d_near.at[k], d_ss.at[k], d_rs.at[k], k))
    for k in by_rows:
        a_copies.append(send(a_send, a_near.at[k], a_ss.at[k], a_rs.at[k], k))

    loads[5].wait()
    local = by_sums + [0]
    mark_near = jnp.concatenate(
        [onehot[partner(kind, k, half)].reshape(2 * padded, width) for k in local], 0).astype(BF16)
    swapped[...] = dot(mark_near, w1[...]).reshape(len(local), 2 * padded, hidden)
    pre_ab = 0.5 * dot(jnp.concatenate([own_a, own_b], 0), w1[...])
    pre_a = pre_ab[:rows]

    def tail(count):
        for c in range(0, hidden, 256):
            h2[:count, c : c + 256] = silu_of_half(0.5 * dot(h1[:count, :], w2[:, c : c + 256])).astype(BF16)
        mid = count // 2 // 16 * 16
        return jnp.concatenate([dot(h2[:mid, :], w3[...]), dot(h2[mid:count, :], w3[...])], 0)

    def fill(base, pre, delta_t, i, groups):
        delta = jnp.transpose(delta_t)
        for g in groups:
            at = (g // gq) * padded + g % gq
            h1[base : base + rows, :] = silu_of_half(
                pre + delta[:, at : at + 1] * swapped[i, at : at + 1, :]).astype(BF16)
            base += rows
        return base

    row_in = lax.broadcasted_iota(jnp.int32, (window_rows, outputs), 0)

    def used(block):
        return jnp.concatenate(
            [(row_in + block * window_rows < ends[w]).astype(F32) for w in range(windows)], 0)

    def by_window(x):
        return jnp.sum(x.reshape(windows, window_rows, outputs), axis=1)

    def spread_rows(x):
        return jnp.concatenate(
            [jnp.broadcast_to(x[w : w + 1], (window_rows, outputs)) for w in range(windows)], 0)

    def count_of(block, w):
        count = jnp.minimum(jnp.maximum(ends[w] - block * window_rows, 0), window_rows)
        return jnp.full((1, outputs), count, jnp.int32).astype(F32)

    everything = range(pg)
    usable = used(me)

    loads[6].wait()
    loads[7].wait()
    base = 0
    for i, k in enumerate(by_sums):
        base = fill(base, pre_a, d_send[partner(kind, k, half)], i, everything)
    h1[base : base + 2 * rows, :] = silu_of_half(pre_ab).astype(BF16)
    out = tail(base + 2 * rows)
    out_a = out[base : base + rows]
    out_b = out[base + rows : base + 2 * rows]
    b_send[...] = out_b
    b_copies = [send(b_send, b_near.at[k], b_ss.at[k], b_rs.at[k], k) for k in by_rows]
    counts = jnp.concatenate([count_of(me, w) for w in range(windows)], 0)
    mean = by_window(usable * (out_a + out_b)) * (0.5 / jnp.maximum(counts, 1.0))
    mean_rows = spread_rows(mean)
    dev_a = out_a - mean_rows
    dev_b = out_b - mean_rows
    shift = by_window(out_b) * (1.0 / window_rows)
    t_all[0] = jnp.concatenate(
        [mean, by_window(usable * (dev_a * dev_a + dev_b * dev_b)), by_window(usable * out_b), shift], 0)
    t_copies = [send(t_all.at[0], t_all.at[k], t_ss.at[k], t_rs.at[k], k) for k in range(n - 1, 0, -1)]
    shift_rows = spread_rows(shift)
    weighted_b = usable * (out_b - shift_rows)
    base = 0
    s_copies = []
    for k in by_sums:
        sums = [[], [], []]
        for g in everything:
            d = out[base : base + rows] - out_a
            base += rows
            masked = usable * d
            for t, term in enumerate((masked, masked * d, weighted_b * d)):
                sums[t].append(term)
        for t in range(3):
            for w in range(windows):
                st_send[k, t, w] = sum_each([x[w * window_rows : (w + 1) * window_rows] for x in sums[t]])
        s_copies.append(send(st_send.at[k], st_near.at[k], s_ss.at[k], s_rs.at[k], k))

    out = tail(fill(0, pre_a, d_send[kind], len(by_sums), everything))
    for g in everything:
        d = out[g * rows : (g + 1) * rows] - out_a
        masked = usable * d
        acc[0, g] = masked
        acc[1, g] = masked * d
        acc[2, g] = weighted_b * d

    for copy in d_copies + a_copies:
        copy.wait_recv()

    x_copies = []
    for stage, (start, stop) in enumerate(stages):
        groups = range(start * gp, stop * gp)
        base = 0
        for i, k in enumerate(by_rows):
            if stage == 0:
                pre_s[i] = 0.5 * dot(a_near[k].astype(BF16), w1[...])
            base = fill(base, pre_s[i], d_near[k], len(by_sums), groups)
            if stage == 0:
                h1[base : base + rows, :] = silu_of_half(pre_s[i]).astype(BF16)
                base += rows
        out = tail(base)
        if stage == 0:
            for copy in b_copies:
                copy.wait_recv()
        base = 0
        for i, k in enumerate(by_rows):
            usable_k = used(partner(me, k, n))
            weighted = usable_k * (b_near[k] - shift_rows)
            if stage == 0:
                oa_s[i] = out[base + len(groups) * rows : base + (len(groups) + 1) * rows]
            out_ak = oa_s[i]
            for g in groups:
                d = out[base : base + rows] - out_ak
                base += rows
                masked = usable_k * d
                acc[0, g] += masked
                acc[1, g] += masked * d
                acc[2, g] += weighted * d
            if stage == 0:
                base += rows
        if stage == 0:
            for copy in t_copies + s_copies:
                copy.wait_recv()
            origin = t_all[0, 3 * windows : 3 * windows + 1]
            blocks = [partner(me, k, n) for k in range(n)]
            former = None
            finish = []
            for w in range(windows):
                count = [count_of(block, w) for block in blocks]
                now_n = sum(count)
                now_mean = sum(c * t_all[k, w : w + 1] for k, c in enumerate(count)) / now_n
                now_spread = sum(t_all[k, windows + w : windows + w + 1] for k in range(n))
                now_spread += 2.0 * sum(c * jnp.square(t_all[k, w : w + 1] - now_mean) for k, c in enumerate(count))
                now_b = sum(t_all[k, 2 * windows + w : 2 * windows + w + 1] for k in range(n))
                if former is not None:
                    n1, m1, s1, b1 = former
                    both = n1 + now_n
                    change = now_mean - m1
                    part = now_n / both
                    now_spread = s1 + now_spread + 2.0 * change * change * n1 * part
                    now_mean = m1 + change * part
                    now_b = b1 + now_b
                    now_n = both
                former = (now_n, now_mean, now_spread, now_b)
                variance = now_spread / (2.0 * now_n)
                variance_ref[w : w + 1] = variance
                finish.append((1.0 / (now_n * variance), now_b / now_n))
        for p in range(start, stop):
            group = range(p * gp, (p + 1) * gp)
            span = slice(p * gp, (p + 1) * gp)

            def block(t, g, w):
                return acc[t, g, w * window_rows : (w + 1) * window_rows]

            sums_dq = sum_each([block(t, g, w) for w in range(windows) for t in range(2) for g in group])
            sums_x = sum_each([block(2, g, w) for w in range(windows) for g in group])
            running = None
            for w in range(windows):
                sum_d = sums_dq[2 * w * gp : (2 * w + 1) * gp]
                sum_q = sums_dq[(2 * w + 1) * gp : (2 * w + 2) * gp]
                sum_x = sums_x[w * gp : (w + 1) * gp]
                sum_x = sum_x + (t_all[0, 3 * windows + w : 3 * windows + w + 1] - origin) * sum_d
                for k in by_sums:
                    d_k = st_near[k, 0, w, span]
                    sum_x = sum_x + st_near[k, 2, w, span]
                    sum_x = sum_x + (t_all[k, 3 * windows + w : 3 * windows + w + 1] - origin) * d_k
                    sum_q = sum_q + st_near[k, 1, w, span]
                    sum_d = sum_d + d_k
                now = (sum_d, sum_q, sum_x)
                running = now if running is None else tuple(x + y for x, y in zip(running, now))
                x_send[p, w, :gp] = running[2] + (origin - finish[w][1]) * running[0]
                x_send[p, w, gp:] = 0.5 * running[1]
            x_copies.append(send(x_send.at[p], x_recv.at[p], x_ss.at[p], x_rs.at[p], half))

    r_copies = []
    for p in range(parts):
        x_copies[p].wait_recv()
        for w in range(windows):
            res[kind, p, w] = (x_send[p, w] + x_recv[p, w]) * finish[w][0]
        mine = res.at[kind, p]
        for k in range(half - 1, 0, -1):
            r_copies.append(send(mine, mine, r_ss.at[p, k], r_rs.at[p, k], k))
    for copy in r_copies:
        copy.wait_recv()
    for copy in copies:
        copy.wait_send()


def deliver(gq, res, variance_ref, first, total, variance):
    half, parts, windows, both, _ = res.shape
    gp = both // 2
    for kind in range(half):
        for w in range(windows):
            for out, span in ((first, slice(0, gp)), (total, slice(gp, both))):
                whole = jnp.concatenate([res[kind, p, w, span] for p in range(parts)], 0)
                out[w, kind * gq : (kind + 1) * gq] = whole[:gq]
                out[w, (half + kind) * gq : (half + kind + 1) * gq] = whole[gq:]
    variance[...] = variance_ref[...]


def solution(mesh):
    n = mesh.shape["rows"]

    def local(base_a, base_b, input_scale, layer_one, layer_two, layer_three, swap_cols, window_ends):
        windows, window_rows, width = base_a.shape
        groups = swap_cols.shape[0]
        gq = groups // n
        pg = 2 * gq
        padded = -(-gq // 8) * 8
        hidden = layer_two.shape[0]
        outputs = layer_three.shape[1]
        rows = windows * window_rows
        half = n // 2
        by_sums, by_rows = near_plan(half)
        gp = part_size(pg)
        parts = pg // gp
        most = rows * max(len(by_sums) * pg + 2, pg, len(by_rows) * (pg - gp + 1))
        hbm = pl.BlockSpec(memory_space=pl.ANY)
        vmem = pl.BlockSpec(memory_space=pltpu.VMEM)
        dma = pltpu.SemaphoreType.DMA
        results = pl.pallas_call(
            functools.partial(kernel, n),
            out_shape=(pltpu.VMEM((half, parts, windows, 2 * gp, outputs), F32), pltpu.VMEM((windows, outputs), F32)),
            in_specs=[hbm] * 8,
            out_specs=(vmem,) * 2,
            scratch_shapes=[
                pltpu.VMEM(base_a.shape, BF16),
                pltpu.VMEM(base_b.shape, BF16),
                pltpu.VMEM((1, width), F32),
                pltpu.SMEM((groups,), jnp.int32),
                pltpu.SMEM((windows,), jnp.int32),
                pltpu.VMEM(layer_one.shape, BF16),
                pltpu.VMEM(layer_two.shape, BF16),
                pltpu.VMEM(layer_three.shape, BF16),
                pltpu.VMEM((rows, width), F32),
                pltpu.VMEM((half, rows, width), F32),
                pltpu.VMEM((half, 2 * padded, rows), F32),
                pltpu.VMEM((half, 2 * padded, rows), F32),
                pltpu.VMEM((half, 2, padded, width), F32),
                pltpu.VMEM((len(by_sums) + 1, 2 * padded, hidden), F32),
                pltpu.VMEM((rows, outputs), F32),
                pltpu.VMEM((half, rows, outputs), F32),
                pltpu.VMEM((n, 4 * windows, outputs), F32),
                pltpu.VMEM((half, 3, windows, pg, outputs), F32),
                pltpu.VMEM((half, 3, windows, pg, outputs), F32),
                pltpu.VMEM((3, pg, rows, outputs), F32),
                pltpu.VMEM((len(by_rows), rows, hidden), F32),
                pltpu.VMEM((len(by_rows), rows, outputs), F32),
                pltpu.VMEM((parts, windows, 2 * gp, outputs), F32),
                pltpu.VMEM((parts, windows, 2 * gp, outputs), F32),
                pltpu.VMEM((most, hidden), BF16),
                pltpu.VMEM((most, hidden), BF16),
                dma((8,)),
            ] + [dma((half,)) for _ in range(8)] + [dma((n,)), dma((n,)), dma((parts,)), dma((parts,)),
                                                    dma((parts, half)), dma((parts, half))],
            compiler_params=pltpu.CompilerParams(
                collective_id=0, has_side_effects=True, vmem_limit_bytes=56 * 2**20
            ),
        )(base_a, base_b, input_scale.reshape(1, width), swap_cols, window_ends,
          layer_one, layer_two, layer_three)
        return pl.pallas_call(
            functools.partial(deliver, gq),
            out_shape=(
                jax.ShapeDtypeStruct((windows, groups, outputs), F32),
                jax.ShapeDtypeStruct((windows, groups, outputs), F32),
                jax.ShapeDtypeStruct((windows, outputs), F32),
            ),
            in_specs=[vmem] * 2,
            out_specs=(vmem, vmem, vmem),
            compiler_params=pltpu.CompilerParams(vmem_limit_bytes=4 * 2**20),
        )(*results)

    in_specs = (P(None, "rows", None), P(None, "rows", None), P(), P(), P(), P(), P("par"), P())
    out_specs = (P(None, "par", None), P(None, "par", None), P())
    return jax.shard_map(local, mesh=mesh, in_specs=in_specs, out_specs=out_specs, check_vma=False)
```

```python
import functools

import jax
import jax.numpy as jnp
from jax import lax
from jax.experimental import pallas as pl
from jax.experimental.pallas import tpu as pltpu
from jax.sharding import PartitionSpec as P

F32 = jnp.float32
BF16 = jnp.bfloat16
MESH = pl.DeviceIdType.MESH


def silu_of_half(half):
    return half + half * jnp.tanh(half)


def dot(x, y):
    return jnp.dot(x, y, preferred_element_type=F32)


def dot_t(x, y):
    return lax.dot_general(x, y, (((1,), (1,)), ((), ())), preferred_element_type=F32)


def partner(me, k, n):
    other = me
    bit = 1
    while bit < n:
        if k & bit:
            other = other + bit - 2 * bit * lax.rem(other // bit, 2)
        bit *= 2
    return other


def near_plan(half):
    cut = half - max(1, half // 4)
    return list(range(half - 1, cut - 1, -1)), list(range(1, cut))


def part_size(count):
    return max(1, count // 4)


def fold(parts):
    row = lax.broadcasted_iota(jnp.int32, parts[0].shape, 0)
    for bit in (4, 2, 1):
        low = (row // bit) % 2 == 0
        merged = []
        for a, b in zip(parts[: len(parts) // 2], parts[len(parts) // 2 :]):
            if bit == 4:
                merged.append(jnp.where(low, a, b) + pltpu.roll(jnp.where(low, b, a), 4, 0))
            else:
                merged.append(jnp.where(low, a + pltpu.roll(a, 8 - bit, 0), b + pltpu.roll(b, bit, 0)))
        parts = merged
    return parts[0]


def sum_each(parts):
    if parts[0].shape[0] != 8 or len(parts) % 8:
        return jnp.concatenate([jnp.sum(x, axis=0, keepdims=True) for x in parts], 0)
    return jnp.concatenate([fold(parts[i : i + 8]) for i in range(0, len(parts), 8)], 0)


def kernel(n, a_hbm, b_hbm, scale_hbm, cols_hbm, ends_hbm, w1_hbm, w2_hbm, w3_hbm,
           res, variance_ref,
           base_a, base_b, scale, cols, ends, w1, w2, w3,
           a_send, a_near, d_send, d_near, onehot, swapped, b_send, b_near, t_all,
           st_send, st_near, acc, pre_s, oa_s, x_send, x_recv, h1, h2,
           in_sems, a_ss, a_rs, d_ss, d_rs, b_ss, b_rs, s_ss, s_rs, t_ss, t_rs, x_ss, x_rs, r_ss, r_rs):
    windows, window_rows, width = base_a.shape
    padded = onehot.shape[2]
    hidden = w2.shape[0]
    outputs = w3.shape[1]
    rows = windows * window_rows
    half = n // 2
    gq = cols.shape[0] // n
    pg = 2 * gq
    by_sums, by_rows = near_plan(half)
    gp = part_size(pg)
    parts = pg // gp
    stages = [(0, parts - 1), (parts - 1, parts)]
    me = lax.axis_index("rows")
    kind = lax.rem(me, half)

    barrier = pltpu.get_barrier_semaphore()
    for k in range(1, n):
        pl.semaphore_signal(barrier, inc=1, device_id={"rows": partner(me, k, n)}, device_id_type=MESH)

    pairs = ((a_hbm, base_a), (b_hbm, base_b), (scale_hbm, scale), (cols_hbm, cols), (ends_hbm, ends),
             (w1_hbm, w1), (w3_hbm, w3))
    quarter = hidden // 4
    pairs += tuple((w2_hbm.at[pl.ds(i * quarter, quarter)], w2.at[pl.ds(i * quarter, quarter)]) for i in range(4))
    loads = [pltpu.make_async_copy(src, dst, in_sems.at[i]) for i, (src, dst) in enumerate(pairs)]
    for load in loads:
        load.start()

    copies = []

    def send(src, dst, ss, rs, k):
        copy = pltpu.make_async_remote_copy(
            src_ref=src, dst_ref=dst, send_sem=ss, recv_sem=rs,
            device_id={"rows": partner(me, k, n)}, device_id_type=MESH)
        copy.start()
        copies.append(copy)
        return copy

    for load in loads[:5]:
        load.wait()
    factor = scale[...]
    own_a32 = (base_a[...].reshape(rows, width).astype(F32) * factor).astype(BF16).astype(F32)
    own_a = own_a32.astype(BF16)
    own_b = (base_b[...].reshape(rows, width).astype(F32) * factor).astype(BF16)
    a_send[...] = own_a32
    loads[5].wait()
    pre_ab = 0.5 * dot(jnp.concatenate([own_a, own_b], 0), w1[...])
    lane = lax.broadcasted_iota(jnp.int32, (padded, width), 1)
    sub = lax.broadcasted_iota(jnp.int32, (padded, width), 0)
    for r in range(n):
        wanted = jnp.full((padded, width), cols[r * gq], jnp.int32)
        for g in range(1, gq):
            wanted = jnp.where(sub == g, cols[r * gq + g], wanted)
        onehot[r % half, r // half] = (lane == wanted).astype(F32)
    marks = onehot[...].reshape(n * padded, width).astype(BF16)
    d_send[...] = (0.5 * (dot_t(marks, own_b) - dot_t(marks, own_a))).reshape(half, 2 * padded, rows)

    pl.semaphore_wait(barrier, n - 1)
    d_copies, a_copies = [], []
    for k in by_rows:
        d_copies.append(send(d_send.at[partner(kind, k, half)], d_near.at[k], d_ss.at[k], d_rs.at[k], k))
    for k in by_rows:
        a_copies.append(send(a_send, a_near.at[k], a_ss.at[k], a_rs.at[k], k))

    local = by_sums + [0]
    mark_near = jnp.concatenate(
        [onehot[partner(kind, k, half)].reshape(2 * padded, width) for k in local], 0).astype(BF16)
    swapped[...] = dot(mark_near, w1[...]).reshape(len(local), 2 * padded, hidden)
    pre_a = pre_ab[:rows]

    def tail(count):
        for c in range(0, hidden, 256):
            h2[:count, c : c + 256] = silu_of_half(0.5 * dot(h1[:count, :], w2[:, c : c + 256])).astype(BF16)
        mid = count // 2 // 16 * 16
        return jnp.concatenate([dot(h2[:mid, :], w3[...]), dot(h2[mid:count, :], w3[...])], 0)

    def fill(base, pre, delta_t, i, groups):
        delta = jnp.transpose(delta_t)
        for g in groups:
            at = (g // gq) * padded + g % gq
            h1[base : base + rows, :] = silu_of_half(
                pre + delta[:, at : at + 1] * swapped[i, at : at + 1, :]).astype(BF16)
            base += rows
        return base

    row_in = lax.broadcasted_iota(jnp.int32, (window_rows, outputs), 0)

    def used(block):
        return jnp.concatenate(
            [(row_in + block * window_rows < ends[w]).astype(F32) for w in range(windows)], 0)

    def by_window(x):
        return jnp.sum(x.reshape(windows, window_rows, outputs), axis=1)

    def spread_rows(x):
        return jnp.concatenate(
            [jnp.broadcast_to(x[w : w + 1], (window_rows, outputs)) for w in range(windows)], 0)

    def count_of(block, w):
        count = jnp.minimum(jnp.maximum(ends[w] - block * window_rows, 0), window_rows)
        return jnp.full((1, outputs), count, jnp.int32).astype(F32)

    everything = range(pg)
    usable = used(me)

    for load in loads[6:]:
        load.wait()
    base = 0
    for i, k in enumerate(by_sums):
        base = fill(base, pre_a, d_send[partner(kind, k, half)], i, everything)
    h1[base : base + 2 * rows, :] = silu_of_half(pre_ab).astype(BF16)
    out = tail(base + 2 * rows)
    out_a = out[base : base + rows]
    out_b = out[base + rows : base + 2 * rows]
    b_send[...] = out_b
    b_copies = [send(b_send, b_near.at[k], b_ss.at[k], b_rs.at[k], k) for k in by_rows]
    counts = jnp.concatenate([count_of(me, w) for w in range(windows)], 0)
    mean = by_window(usable * (out_a + out_b)) * (0.5 / jnp.maximum(counts, 1.0))
    mean_rows = spread_rows(mean)
    dev_a = out_a - mean_rows
    dev_b = out_b - mean_rows
    shift = by_window(out_b) * (1.0 / window_rows)
    t_all[0] = jnp.concatenate(
        [mean, by_window(usable * (dev_a * dev_a + dev_b * dev_b)), by_window(usable * out_b), shift], 0)
    t_copies = [send(t_all.at[0], t_all.at[k], t_ss.at[k], t_rs.at[k], k) for k in range(n - 1, 0, -1)]
    shift_rows = spread_rows(shift)
    weighted_b = usable * (out_b - shift_rows)
    base = 0
    s_copies = []
    for k in by_sums:
        sums = [[], [], []]
        for g in everything:
            d = out[base : base + rows] - out_a
            base += rows
            masked = usable * d
            for t, term in enumerate((masked, masked * d, weighted_b * d)):
                sums[t].append(term)
        for t in range(3):
            for w in range(windows):
                st_send[k, t, w] = sum_each([x[w * window_rows : (w + 1) * window_rows] for x in sums[t]])
        s_copies.append(send(st_send.at[k], st_near.at[k], s_ss.at[k], s_rs.at[k], k))

    out = tail(fill(0, pre_a, d_send[kind], len(by_sums), everything))
    for g in everything:
        d = out[g * rows : (g + 1) * rows] - out_a
        masked = usable * d
        acc[0, g] = masked
        acc[1, g] = masked * d
        acc[2, g] = weighted_b * d

    for copy in d_copies + a_copies:
        copy.wait_recv()

    x_copies = []
    for stage, (start, stop) in enumerate(stages):
        groups = range(start * gp, stop * gp)
        base = 0
        for i, k in enumerate(by_rows):
            if stage == 0:
                pre_s[i] = 0.5 * dot(a_near[k].astype(BF16), w1[...])
            base = fill(base, pre_s[i], d_near[k], len(by_sums), groups)
            if stage == 0:
                h1[base : base + rows, :] = silu_of_half(pre_s[i]).astype(BF16)
                base += rows
        out = tail(base)
        if stage == 0:
            for copy in b_copies:
                copy.wait_recv()
        base = 0
        for i, k in enumerate(by_rows):
            usable_k = used(partner(me, k, n))
            weighted = usable_k * (b_near[k] - shift_rows)
            if stage == 0:
                oa_s[i] = out[base + len(groups) * rows : base + (len(groups) + 1) * rows]
            out_ak = oa_s[i]
            for g in groups:
                d = out[base : base + rows] - out_ak
                base += rows
                masked = usable_k * d
                acc[0, g] += masked
                acc[1, g] += masked * d
                acc[2, g] += weighted * d
            if stage == 0:
                base += rows
        if stage == 0:
            for copy in t_copies + s_copies:
                copy.wait_recv()
            origin = t_all[0, 3 * windows : 3 * windows + 1]
            blocks = [partner(me, k, n) for k in range(n)]
            former = None
            finish = []
            for w in range(windows):
                count = [count_of(block, w) for block in blocks]
                now_n = sum(count)
                now_mean = sum(c * t_all[k, w : w + 1] for k, c in enumerate(count)) / now_n
                now_spread = sum(t_all[k, windows + w : windows + w + 1] for k in range(n))
                now_spread += 2.0 * sum(c * jnp.square(t_all[k, w : w + 1] - now_mean) for k, c in enumerate(count))
                now_b = sum(t_all[k, 2 * windows + w : 2 * windows + w + 1] for k in range(n))
                if former is not None:
                    n1, m1, s1, b1 = former
                    both = n1 + now_n
                    change = now_mean - m1
                    part = now_n / both
                    now_spread = s1 + now_spread + 2.0 * change * change * n1 * part
                    now_mean = m1 + change * part
                    now_b = b1 + now_b
                    now_n = both
                former = (now_n, now_mean, now_spread, now_b)
                variance = now_spread / (2.0 * now_n)
                variance_ref[w : w + 1] = variance
                finish.append((1.0 / (now_n * variance), now_b / now_n))
        for p in range(start, stop):
            group = range(p * gp, (p + 1) * gp)
            span = slice(p * gp, (p + 1) * gp)

            def block(t, g, w):
                return acc[t, g, w * window_rows : (w + 1) * window_rows]

            sums_dq = sum_each([block(t, g, w) for w in range(windows) for t in range(2) for g in group])
            sums_x = sum_each([block(2, g, w) for w in range(windows) for g in group])
            running = None
            for w in range(windows):
                sum_d = sums_dq[2 * w * gp : (2 * w + 1) * gp]
                sum_q = sums_dq[(2 * w + 1) * gp : (2 * w + 2) * gp]
                sum_x = sums_x[w * gp : (w + 1) * gp]
                sum_x = sum_x + (t_all[0, 3 * windows + w : 3 * windows + w + 1] - origin) * sum_d
                for k in by_sums:
                    d_k = st_near[k, 0, w, span]
                    sum_x = sum_x + st_near[k, 2, w, span]
                    sum_x = sum_x + (t_all[k, 3 * windows + w : 3 * windows + w + 1] - origin) * d_k
                    sum_q = sum_q + st_near[k, 1, w, span]
                    sum_d = sum_d + d_k
                now = (sum_d, sum_q, sum_x)
                running = now if running is None else tuple(x + y for x, y in zip(running, now))
                x_send[p, w, :gp] = running[2] + (origin - finish[w][1]) * running[0]
                x_send[p, w, gp:] = 0.5 * running[1]
            x_copies.append(send(x_send.at[p], x_recv.at[p], x_ss.at[p], x_rs.at[p], half))

    r_copies = []
    for p in range(parts):
        x_copies[p].wait_recv()
        for w in range(windows):
            res[kind, p, w] = (x_send[p, w] + x_recv[p, w]) * finish[w][0]
        mine = res.at[kind, p]
        for k in range(half - 1, 0, -1):
            r_copies.append(send(mine, mine, r_ss.at[p, k], r_rs.at[p, k], k))
    for copy in r_copies:
        copy.wait_recv()
    for copy in copies:
        copy.wait_send()


def deliver(gq, res, variance_ref, first_out, total_out, variance_out, first, total, sems):
    half, parts, windows, both, _ = res.shape
    gp = both // 2
    copies = [pltpu.make_async_copy(variance_ref, variance_out, sems.at[0])]
    copies[0].start()
    for i, (block, target, span) in enumerate(((first, first_out, slice(0, gp)), (total, total_out, slice(gp, both)))):
        for w in range(windows):
            for kind in range(half):
                whole = jnp.concatenate([res[kind, p, w, span] for p in range(parts)], 0)
                block[w, kind * gq : (kind + 1) * gq] = whole[:gq]
                block[w, (half + kind) * gq : (half + kind + 1) * gq] = whole[gq:]
        copies.append(pltpu.make_async_copy(block, target, sems.at[1 + i]))
        copies[-1].start()
    for copy in copies:
        copy.wait()


def solution(mesh):
    n = mesh.shape["rows"]

    def local(base_a, base_b, input_scale, layer_one, layer_two, layer_three, swap_cols, window_ends):
        windows, window_rows, width = base_a.shape
        groups = swap_cols.shape[0]
        gq = groups // n
        pg = 2 * gq
        padded = -(-gq // 8) * 8
        hidden = layer_two.shape[0]
        outputs = layer_three.shape[1]
        rows = windows * window_rows
        half = n // 2
        by_sums, by_rows = near_plan(half)
        gp = part_size(pg)
        parts = pg // gp
        most = rows * max(len(by_sums) * pg + 2, pg, len(by_rows) * (pg - gp + 1))
        hbm = pl.BlockSpec(memory_space=pl.ANY)
        vmem = pl.BlockSpec(memory_space=pltpu.VMEM)
        dma = pltpu.SemaphoreType.DMA
        results = pl.pallas_call(
            functools.partial(kernel, n),
            out_shape=(pltpu.VMEM((half, parts, windows, 2 * gp, outputs), F32), pltpu.VMEM((windows, outputs), F32)),
            in_specs=[hbm] * 8,
            out_specs=(vmem,) * 2,
            scratch_shapes=[
                pltpu.VMEM(base_a.shape, BF16),
                pltpu.VMEM(base_b.shape, BF16),
                pltpu.VMEM((1, width), F32),
                pltpu.SMEM((groups,), jnp.int32),
                pltpu.SMEM((windows,), jnp.int32),
                pltpu.VMEM(layer_one.shape, BF16),
                pltpu.VMEM(layer_two.shape, BF16),
                pltpu.VMEM(layer_three.shape, BF16),
                pltpu.VMEM((rows, width), F32),
                pltpu.VMEM((half, rows, width), F32),
                pltpu.VMEM((half, 2 * padded, rows), F32),
                pltpu.VMEM((half, 2 * padded, rows), F32),
                pltpu.VMEM((half, 2, padded, width), F32),
                pltpu.VMEM((len(by_sums) + 1, 2 * padded, hidden), F32),
                pltpu.VMEM((rows, outputs), F32),
                pltpu.VMEM((half, rows, outputs), F32),
                pltpu.VMEM((n, 4 * windows, outputs), F32),
                pltpu.VMEM((half, 3, windows, pg, outputs), F32),
                pltpu.VMEM((half, 3, windows, pg, outputs), F32),
                pltpu.VMEM((3, pg, rows, outputs), F32),
                pltpu.VMEM((len(by_rows), rows, hidden), F32),
                pltpu.VMEM((len(by_rows), rows, outputs), F32),
                pltpu.VMEM((parts, windows, 2 * gp, outputs), F32),
                pltpu.VMEM((parts, windows, 2 * gp, outputs), F32),
                pltpu.VMEM((most, hidden), BF16),
                pltpu.VMEM((most, hidden), BF16),
                dma((11,)),
            ] + [dma((half,)) for _ in range(8)] + [dma((n,)), dma((n,)), dma((parts,)), dma((parts,)),
                                                    dma((parts, half)), dma((parts, half))],
            compiler_params=pltpu.CompilerParams(
                collective_id=0, has_side_effects=True, vmem_limit_bytes=56 * 2**20
            ),
        )(base_a, base_b, input_scale.reshape(1, width), swap_cols, window_ends,
          layer_one, layer_two, layer_three)
        return pl.pallas_call(
            functools.partial(deliver, gq),
            out_shape=(
                jax.ShapeDtypeStruct((windows, groups, outputs), F32),
                jax.ShapeDtypeStruct((windows, groups, outputs), F32),
                jax.ShapeDtypeStruct((windows, outputs), F32),
            ),
            in_specs=[vmem] * 2,
            out_specs=(hbm, hbm, hbm),
            scratch_shapes=[
                pltpu.VMEM((windows, groups, outputs), F32),
                pltpu.VMEM((windows, groups, outputs), F32),
                dma((3,)),
            ],
            compiler_params=pltpu.CompilerParams(vmem_limit_bytes=4 * 2**20),
        )(*results)

    in_specs = (P(None, "rows", None), P(None, "rows", None), P(), P(), P(), P(), P("par"), P())
    out_specs = (P(None, "par", None), P(None, "par", None), P())
    return jax.shard_map(local, mesh=mesh, in_specs=in_specs, out_specs=out_specs, check_vma=False)
```
